32 devices in a mesh: seq: 8 (over z, y), grp: 4 (over x, core).
Axes of the slice: x: 2, y: 2, z: 4, core: 2. Of those that a mesh axis runs over, the one named last changes fastest.
Arguments:
- hidden: bfloat16 [4096, 2048], P('seq', 'grp'), may hold values from -8 to 8
- qkv_weight: bfloat16 [3, 2048, 6144], P(None, 'seq', 'grp'), may hold values from -0.125 to 0.125
- out_weight: bfloat16 [3, 2048, 2048], P(None, 'grp', 'seq'), may hold values from -0.125 to 0.125
- projection: float32 [3, 16, 128, 128], P(None, 'grp'), may hold values from -6 to 6
- norm_gain: float32 [3, 2048], replicated, may hold values from 0.1 to 1.9
- out_gain: float32 [3, 2048], P(None, 'grp'), may hold values from 0.1 to 1.9
Outputs:
- layer_out: bfloat16 [4096, 2048], P('seq', 'grp')
The draws below stay inside these ranges and needn't reach their ends.
All inputs are finite; a program needn't handle non-finite values.
Results may differ from the reference program's by a relative error of at most 0.034.
Values may be sent and summed in bfloat16 or wider, within the bound.
A program may use at most 64 MiB of HBM per device.

```python
import math
import jax
import jax.numpy as jnp
from jax import lax

D = 2048
H = 16
E = 128
M = 128
LAYERS = 3
TOK_DEV = 512
TOKENS = 4096
N_GRP = 4


def draw_hidden(key, part):
    base = jax.random.normal(jax.random.fold_in(key, 11), (TOKENS, D), jnp.float32)
    return jnp.clip(base, -8.0, 8.0).astype(jnp.bfloat16)


def block_scale(key, extent, shards, least, high):
    gain = 1.0
    for position, blocks in shards:
        heights = jax.random.uniform(jax.random.fold_in(jax.random.fold_in(key, 6), position), (blocks,), jnp.float32, least / len(shards), high / len(shards))
        gain = gain * jnp.repeat(jnp.exp(heights), extent[position] // blocks).reshape((-1,) + (1,) * (len(extent) - 1 - position))
    return gain


def normal_values(key, shape, scale, limit, pieces=(), held_as=jnp.bfloat16):
    gain = block_scale(key, shape, pieces, -0.22, 0.18) if pieces else 1.0
    drawn = jax.random.normal(key, shape, jnp.float32) * scale * gain
    return jnp.minimum(jnp.maximum(drawn, -limit), limit).astype(held_as)


def setup_inputs(seed: int = 0) -> dict:
    splits = jax.random.split(jax.random.key(seed), 7)
    hidden = draw_hidden(jax.random.fold_in(splits[6], 71), 0)
    qkv_weight = normal_values(splits[1], (LAYERS, D, 3 * H * E), D ** -0.5, 0.125, ((1, 8), (2, 4)))
    out_weight = normal_values(splits[2], (LAYERS, H * E, D), (H * E) ** -0.5, 0.125, ((1, 4), (2, 8)))
    projection = normal_values(splits[3], (LAYERS, H, E, M), 1.0, 6.0, ((1, 4),), jnp.float32)
    norm_gain = jnp.clip(1.0 + 0.18 * jax.random.normal(splits[4], (LAYERS, D), jnp.float32), 0.1, 1.9)
    out_gain = jnp.clip(1.0 + 0.18 * jax.random.normal(splits[5], (LAYERS, H * E), jnp.float32), 0.1, 1.9)
    return {"hidden": hidden, "qkv_weight": qkv_weight, "out_weight": out_weight, "projection": projection, "norm_gain": norm_gain, "out_gain": out_gain}


stabilizer = 2.0
highest = lax.Precision.HIGHEST

def features(rows, projection_layer):
    scaled = rows.astype(jnp.float32) * E ** (-0.25)
    mixed = jnp.einsum('thd,hdm->thm', scaled, projection_layer, precision=highest)
    energy = 0.5 * lax.optimization_barrier(jnp.sum(scaled * scaled, axis=-1, keepdims=True))
    return (jnp.exp(mixed - energy - stabilizer) / math.sqrt(M)).astype(jnp.bfloat16)

def block_step(carried, block):
    prefix_kv, prefix_z = carried
    query_feat, key_feat, value_rows = block
    query_wide = query_feat.astype(jnp.float32)
    key_wide = key_feat.astype(jnp.float32)
    value_wide = value_rows.astype(jnp.float32)
    scores = jnp.einsum('ihm,jhm->hij', query_wide, key_wide, precision=highest)
    count = scores.shape[-1]
    causal_mask = jnp.arange(count)[:, None] >= jnp.arange(count)[None, :]
    masked = jnp.where(causal_mask[None], scores, jnp.zeros_like(scores))
    score_weights = lax.optimization_barrier(masked.astype(jnp.bfloat16)).astype(jnp.float32)
    rounded_kv = lax.optimization_barrier(prefix_kv.astype(jnp.bfloat16)).astype(jnp.float32)
    denominator = lax.optimization_barrier(jnp.sum(masked, axis=-1)) + jnp.einsum('ihm,hm->hi', query_wide, prefix_z, precision=highest)
    numerator = jnp.einsum('hij,jhe->hie', score_weights, value_wide, precision=highest)
    numerator = numerator + jnp.einsum('ihm,hme->hie', query_wide, rounded_kv, precision=highest)
    attention = numerator / denominator[..., None]
    block_kv = jnp.einsum('jhm,jhe->hme', key_wide, value_wide, precision=highest)
    block_z = lax.optimization_barrier(jnp.sum(key_wide, axis=0))
    return ((prefix_kv + block_kv, prefix_z + block_z), jnp.transpose(attention, (1, 0, 2)))

def reference(hidden, qkv_weight, out_weight, projection, norm_gain, out_gain):
    stream = hidden
    blocks = TOKENS // TOK_DEV
    group_cols = H // N_GRP * E
    for layer_index in range(LAYERS):
        wide = stream.astype(jnp.float32)
        inverse_rms = lax.rsqrt(lax.optimization_barrier(jnp.mean(wide * wide, axis=-1, keepdims=True)) + 1e-05)
        normed = (wide * inverse_rms * norm_gain[layer_index][None, :]).astype(jnp.bfloat16)
        qkv = jnp.dot(normed, qkv_weight[layer_index], preferred_element_type=jnp.float32).astype(jnp.bfloat16)
        qkv = qkv.reshape(TOKENS, H, 3, E)
        query_feat = features(qkv[:, :, 0], projection[layer_index])
        key_feat = features(qkv[:, :, 1], projection[layer_index])
        value_rows = qkv[:, :, 2]
        start_state = (jnp.zeros((H, M, E), jnp.float32), jnp.zeros((H, M), jnp.float32))
        packed = (query_feat.reshape(blocks, TOK_DEV, H, M), key_feat.reshape(blocks, TOK_DEV, H, M), value_rows.reshape(blocks, TOK_DEV, H, E))
        final_state, attention = lax.scan(block_step, start_state, packed)
        attention = attention.reshape(TOKENS, H, E)
        inverse_norm = lax.rsqrt(lax.optimization_barrier(jnp.mean(attention * attention, axis=-1, keepdims=True)) + 1e-06)
        attended = (attention * inverse_norm * out_gain[layer_index].reshape(H, E)[None]).astype(jnp.bfloat16)
        attended = attended.reshape(TOKENS, H * E)
        summed = jnp.zeros((TOKENS, D), jnp.float32)
        for group_index in range(N_GRP):
            lower = group_index * group_cols
            partial_value = jnp.dot(attended[:, lower:lower + group_cols], out_weight[layer_index][lower:lower + group_cols], preferred_element_type=jnp.float32)
            summed = summed + lax.optimization_barrier(partial_value.astype(jnp.bfloat16)).astype(jnp.float32)
        stream = (stream.astype(jnp.float32) + summed).astype(jnp.bfloat16)
    return stream
```

```python
import functools
import math

import jax
import jax.numpy as jnp
from jax import lax
from jax.experimental import pallas as pl
from jax.experimental.pallas import tpu as pltpu
from jax.sharding import PartitionSpec as P

MESH = pl.DeviceIdType.MESH
stabilizer = 2.0
f32 = jnp.float32
bf16 = jnp.bfloat16


def remote(src, dst, send, recv, device):
    return pltpu.make_async_remote_copy(
        src_ref=src, dst_ref=dst, send_sem=send, recv_sem=recv, device_id=device, device_id_type=MESH
    )


def kernel(
    n_seq, n_grp, hidden, qkv_w, out_w, proj, norm_gain, out_gain, out,
    wq, wo, xg, part, rs, normed, qf, kf, vf, num, den, att,
    own_state, st_send, st_pair, ps_send, st_line, prefix,
    local_sem, z_send, z_recv, y_send, y_recv, p_send, p_recv, l_send, l_recv,
    ag_send, ag_recv, rs_send, rs_recv,
):
    layers, rows, cols = qkv_w.shape
    oc = out_w.shape[2]
    tokens, width = hidden.shape
    heads = proj.shape[1]
    head = proj.shape[2]
    feats = proj.shape[3] // 3
    lines = n_seq // 2
    me = lax.axis_index("seq")
    grp = lax.axis_index("grp")
    line, parity = me // 2, me % 2
    pair = line * 2 + 1 - parity

    stores = ((qkv_w, wq), (out_w, wo))
    own_copies = [
        [pltpu.make_async_copy(src.at[l], dst.at[l, me], local_sem.at[1 + 2 * l + k]) for k, (src, dst) in enumerate(stores)]
        for l in range(layers)
    ]
    own_hidden = pltpu.make_async_copy(hidden, xg.at[grp], local_sem.at[0])
    own_hidden.start()
    for pair_copies in own_copies:
        for c in pair_copies:
            c.start()

    barrier = pltpu.get_barrier_semaphore()
    for k in range(1, lines):
        pl.semaphore_signal(barrier, inc=1, device_id={"seq": lax.rem(line + k, lines) * 2 + parity}, device_id_type=MESH)
    pl.semaphore_signal(barrier, inc=1, device_id={"seq": pair}, device_id_type=MESH)
    for k in range(1, n_grp):
        pl.semaphore_signal(barrier, inc=1, device_id={"grp": lax.rem(grp + k, n_grp)}, device_id_type=MESH)
    pl.semaphore_wait(barrier, lines + n_grp - 1)

    def z_copy(l, k, step):
        ref = stores[k][1].at[l, me]
        to = lax.rem(line + step, lines) * 2 + parity
        return remote(ref, ref, z_send.at[l, k, step], z_recv.at[l, k, line], {"seq": to})

    def z_arrival(l, k, step):
        src = lax.rem(line + lines - step, lines)
        ref = stores[k][1].at[l, src * 2 + parity]
        return remote(ref, ref, z_send.at[l, k, step], z_recv.at[l, k, src], {"seq": src * 2 + parity})

    def y_copy(l, k, step):
        src = lax.rem(line + lines - step, lines)
        ref = stores[k][1].at[l, src * 2 + parity]
        return remote(ref, ref, y_send.at[l, k, src], y_recv.at[l, k, src], {"seq": pair})

    def y_arrival(l, k, step):
        src = lax.rem(line + lines - step, lines)
        ref = stores[k][1].at[l, src * 2 + 1 - parity]
        return remote(ref, ref, y_send.at[l, k, src], y_recv.at[l, k, src], {"seq": pair})

    def send_weights(l, k):
        own_copies[l][k].wait()
        for step in range(1, lines):
            z_copy(l, k, step).start()
        y_copy(l, k, 0).start()

    def forward(l, k, step):
        z_arrival(l, k, step).wait_recv()
        y_copy(l, k, step).start()

    def ag_copy(l, k):
        to = lax.rem(grp + k, n_grp)
        return remote(xg.at[grp], xg.at[grp], ag_send.at[l, k], ag_recv.at[l, grp], {"grp": to})

    def ag_arrival(l, k):
        src = lax.rem(grp + k, n_grp)
        return remote(xg.at[src], xg.at[src], ag_send.at[l, k], ag_recv.at[l, src], {"grp": src})

    def rs_copy(l, k):
        to = lax.rem(grp + k, n_grp)
        return remote(part.at[to], rs.at[grp], rs_send.at[l, k], rs_recv.at[l, grp], {"grp": to})

    def rs_arrival(l, k):
        src = lax.rem(grp + k, n_grp)
        return remote(part.at[src], rs.at[src], rs_send.at[l, k], rs_recv.at[l, src], {"grp": src})

    def pair_copy(l):
        return remote(st_send.at[l], st_pair.at[l], p_send.at[l], p_recv.at[l], {"seq": pair})

    def line_copy(l, step):
        return remote(
            ps_send.at[l], st_line.at[l, line], l_send.at[l, step], l_recv.at[l, line],
            {"seq": lax.rem(line + step, lines) * 2 + parity},
        )

    def line_arrival(l, step):
        src = lax.rem(line + lines - step, lines)
        return remote(ps_send.at[l], st_line.at[l, src], l_send.at[l, step], l_recv.at[l, src], {"seq": src * 2 + parity})

    own_hidden.wait()
    for k in range(1, n_grp):
        ag_copy(0, k).start()
    send_weights(0, 0)
    send_weights(0, 1)

    scale = head ** (-0.25)
    inv = 1.0 / math.sqrt(feats)

    def features(u, terms):
        mixed = jnp.dot(u, terms, preferred_element_type=f32)
        mixed = (mixed[:, 2 * feats :] + mixed[:, feats : 2 * feats]) + mixed[:, :feats]
        w0 = u.astype(f32) * scale
        energy = 0.5 * jnp.sum(w0 * w0, axis=-1, keepdims=True)
        return (jnp.exp(mixed - energy - stabilizer) * inv).astype(bf16)

    forwarded = 0
    for l in range(layers):
        last = l == layers - 1
        for k in range(1, n_grp):
            ag_copy(l, k).wait_send()
            ag_arrival(l, k).wait_recv()

        @pl.loop(0, tokens // 64)
        def _(t):
            at = pl.ds(pl.multiple_of(t * 64, 64), 64)
            wide = [xg[g, at, :].astype(f32) for g in range(n_grp)]
            total = sum(jnp.sum(v * v, axis=-1, keepdims=True) for v in wide)
            rms = lax.rsqrt(total / (width * n_grp) + 1e-05)
            for g in range(n_grp):
                cut = slice(g * width, (g + 1) * width)
                normed[at, cut] = (wide[g] * rms * norm_gain[l : l + 1, cut]).astype(bf16)

        for step in range(1 + forwarded, lines):
            forward(l, 0, step)
        for step in range(lines):
            y_arrival(l, 0, step).wait_recv()

        @pl.loop(0, heads)
        def _(h):
            at = pl.ds(pl.multiple_of(h * 3 * head, 128), 3 * head)
            w = wq[l, :, :, at].reshape(n_seq * rows, 3 * head)
            qkv = jnp.dot(normed[...], w, preferred_element_type=f32).astype(bf16)
            terms = proj[l, h]
            key = features(qkv[:, head : 2 * head], terms)
            value = qkv[:, 2 * head :]
            qf[h] = features(qkv[:, :head], terms)
            kf[h] = key
            vf[h] = value
            kv = lax.dot_general(key, value, (((0,), (0,)), ((), ())), preferred_element_type=f32)
            z = jnp.dot(jnp.ones((16, tokens), bf16), key, preferred_element_type=f32)
            own_state[h, :feats] = kv
            own_state[h, feats:] = z
            st_send[l, h, :feats] = kv.astype(bf16)
            st_send[l, h, feats:] = z.astype(bf16)

        pair_copy(l).start()
        for step in range(1, lines):
            forward(l, 1, step)
        pair_copy(l).wait_recv()

        @pl.loop(0, heads)
        def _(h):
            ps_send[l, h] = (own_state[h] + st_pair[l, h].astype(f32)).astype(bf16)

        for step in range(1, lines):
            @pl.when(line + step < lines)
            def _(step=step):
                line_copy(l, step).start()

        if not last:
            send_weights(l + 1, 0)
            send_weights(l + 1, 1)

        @pl.loop(0, heads)
        def _(h):
            scores = lax.dot_general(qf[h], kf[h], (((1,), (1,)), ((), ())), preferred_element_type=f32)
            r = lax.broadcasted_iota(jnp.int32, (tokens, tokens), 0)
            c = lax.broadcasted_iota(jnp.int32, (tokens, tokens), 1)
            masked = jnp.where(r >= c, scores, 0.0)
            den[h] = jnp.broadcast_to(jnp.sum(masked, axis=-1, keepdims=True), (tokens, head))
            num[h] = jnp.dot(masked.astype(bf16), vf[h], preferred_element_type=f32)

        odd = jnp.where(parity == 1, 1.0, 0.0)

        @pl.loop(0, heads)
        def _(h):
            prefix[h] = st_pair[l, h].astype(f32) * odd

        for step in range(1, lines):
            @pl.when(line >= step)
            def _(step=step):
                line_arrival(l, step).wait_recv()
                src = lax.rem(line + lines - step, lines)

                @pl.loop(0, heads)
                def _(h):
                    prefix[h] = prefix[h] + st_line[l, src, h].astype(f32)

        @pl.loop(0, heads)
        def _(h):
            q = qf[h]
            z = prefix[h, feats : feats + 1]
            d = den[h] + jnp.sum(q.astype(f32) * z, axis=-1, keepdims=True)
            n = num[h] + jnp.dot(q, prefix[h, :feats].astype(bf16), preferred_element_type=f32)
            a = n / d
            norm = lax.rsqrt(jnp.mean(a * a, axis=-1, keepdims=True) + 1e-06)
            att[:, pl.ds(pl.multiple_of(h * head, 128), head)] = (a * norm * out_gain[l, h]).astype(bf16)

        for step in range(lines):
            y_arrival(l, 1, step).wait_recv()
        per = width // oc
        for k in list(range(1, n_grp)) + [0]:
            to = lax.rem(grp + k, n_grp)
            for i in range(per):
                part[to, :, i * oc : (i + 1) * oc] = jnp.dot(
                    att[...], wo[l, to * per + i], preferred_element_type=f32
                ).astype(bf16)
            if k:
                rs_copy(l, k).start()
        forwarded = 0
        if not last and lines > 1:
            forward(l + 1, 0, 1)
            forwarded = 1
        for k in range(1, n_grp):
            rs_copy(l, k).wait_send()
            rs_arrival(l, k).wait_recv()

        @pl.loop(0, tokens // 64)
        def _(t):
            at = pl.ds(pl.multiple_of(t * 64, 64), 64)
            total = part[grp, at, :].astype(f32)
            for k in range(1, n_grp):
                total = total + rs[lax.rem(grp + k, n_grp), at, :].astype(f32)
            total = (xg[grp, at, :].astype(f32) + total).astype(bf16)
            if last:
                out[at, :] = total
            else:
                xg[grp, at, :] = total

        if not last:
            for k in range(1, n_grp):
                ag_copy(l + 1, k).start()
            if lines > 2:
                forward(l + 1, 0, 2)
                forwarded = 2

    for l in range(layers):
        pair_copy(l).wait_send()
        for k in range(2):
            for step in range(1, lines):
                z_copy(l, k, step).wait_send()
            for step in range(lines):
                y_copy(l, k, step).wait_send()
        for step in range(1, lines):
            @pl.when(line + step < lines)
            def _(step=step):
                line_copy(l, step).wait_send()


def local(n_seq, n_grp, hidden, qkv_weight, out_weight, projection, norm_gain, out_gain):
    layers, rows, cols = qkv_weight.shape
    depth, oc = out_weight.shape[1:]
    heads, head, feats = projection.shape[1:]
    tokens, width = hidden.shape
    lines = n_seq // 2
    scaled = projection * head ** (-0.25)
    high = lax.reduce_precision(scaled, 8, 7)
    rest = scaled - high
    mid = lax.reduce_precision(rest, 8, 7)
    low = rest - mid
    terms = jnp.concatenate([high, mid, low], axis=-1).astype(bf16)
    gains = out_gain.reshape(layers, heads, 1, head)
    dma = pltpu.SemaphoreType.DMA
    vmem = pl.BlockSpec(memory_space=pltpu.VMEM)
    anywhere = pl.BlockSpec(memory_space=pl.ANY)
    state = (heads, feats + 16, head)
    return pl.pallas_call(
        functools.partial(kernel, n_seq, n_grp),
        out_shape=jax.ShapeDtypeStruct((tokens, width), bf16),
        in_specs=[anywhere, anywhere, anywhere, vmem, vmem, vmem],
        out_specs=vmem,
        scratch_shapes=[
            pltpu.VMEM((layers, n_seq, rows, cols), bf16),
            pltpu.VMEM((layers, n_seq, depth, oc), bf16),
            pltpu.VMEM((n_grp, tokens, width), bf16),
            pltpu.VMEM((n_grp, tokens, width), bf16),
            pltpu.VMEM((n_grp, tokens, width), bf16),
            pltpu.VMEM((tokens, n_grp * width), bf16),
            pltpu.VMEM((heads, tokens, feats), bf16),
            pltpu.VMEM((heads, tokens, feats), bf16),
            pltpu.VMEM((heads, tokens, head), bf16),
            pltpu.VMEM((heads, tokens, head), f32),
            pltpu.VMEM((heads, tokens, head), f32),
            pltpu.VMEM((tokens, heads * head), bf16),
            pltpu.VMEM(state, f32),
            pltpu.VMEM((layers,) + state, bf16),
            pltpu.VMEM((layers,) + state, bf16),
            pltpu.VMEM((layers,) + state, bf16),
            pltpu.VMEM((layers, lines) + state, bf16),
            pltpu.VMEM(state, f32),
            dma((1 + 2 * layers,)),
            dma((layers, 2, lines)),
            dma((layers, 2, lines)),
            dma((layers, 2, lines)),
            dma((layers, 2, lines)),
            dma((layers,)),
            dma((layers,)),
            dma((layers, lines)),
            dma((layers, lines)),
            dma((layers, n_grp)),
            dma((layers, n_grp)),
            dma((layers, n_grp)),
            dma((layers, n_grp)),
        ],
        compiler_params=pltpu.CompilerParams(
            collective_id=0, has_side_effects=True, vmem_limit_bytes=66_000_000
        ),
    )(hidden, qkv_weight, out_weight, terms, norm_gain, gains)


def solution(mesh):
    return jax.shard_map(
        functools.partial(local, mesh.shape["seq"], mesh.shape["grp"]),
        mesh=mesh,
        in_specs=(
            P("seq", "grp"),
            P(None, "seq", "grp"),
            P(None, "grp", "seq"),
            P(None, "grp", None, None),
            P(),
            P(None, "grp"),
        ),
        out_specs=P("seq", "grp"),
        check_vma=False,
    )
```

```python
import functools
import math

import jax
import jax.numpy as jnp
from jax import lax
from jax.experimental import pallas as pl
from jax.experimental.pallas import tpu as pltpu
from jax.sharding import PartitionSpec as P

MESH = pl.DeviceIdType.MESH
stabilizer = 2.0
f32 = jnp.float32
bf16 = jnp.bfloat16


def remote(src, dst, send, recv, device):
    return pltpu.make_async_remote_copy(
        src_ref=src, dst_ref=dst, send_sem=send, recv_sem=recv, device_id=device, device_id_type=MESH
    )


def exchange(line, step, lines):
    if lines & (lines - 1):
        return lax.rem(line + step, lines), lax.rem(line + lines - step, lines)
    other, bit = line, 1
    while bit < lines:
        if step & bit:
            other = other + bit * (1 - 2 * ((line // bit) % 2))
        bit *= 2
    return other, other


def kernel(
    n_seq, n_grp, hidden, qkv_w, out_w, proj, norm_gain, out_gain, out,
    wq, wo, xg, part, rs, normed, qf, kf, vf, num, den, att,
    own_state, st_send, st_pair, ps_send, st_line, prefix,
    local_sem, z_send, z_recv, y_send, y_recv, p_send, p_recv, l_send, l_recv,
    ag_send, ag_recv, rs_send, rs_recv,
):
    layers, rows, cols = qkv_w.shape
    oc = out_w.shape[2]
    tokens, width = hidden.shape
    heads = proj.shape[1]
    head = proj.shape[2]
    feats = proj.shape[3] // 3
    lines = n_seq // 2
    me = lax.axis_index("seq")
    grp = lax.axis_index("grp")
    line, parity = me // 2, me % 2
    pair = line * 2 + 1 - parity

    stores = ((qkv_w, wq), (out_w, wo))
    halves = 2
    cut_rows = rows // halves

    def piece(l, k, owner):
        if k == halves:
            return wo.at[l, owner]
        return wq.at[l, owner, pl.ds(k * cut_rows, cut_rows)]

    own_copies = [
        [pltpu.make_async_copy(src.at[l], dst.at[l, me], local_sem.at[1 + 2 * l + k]) for k, (src, dst) in enumerate(stores)]
        for l in range(layers)
    ]
    own_hidden = pltpu.make_async_copy(hidden, xg.at[grp], local_sem.at[0])
    own_hidden.start()
    for pair_copies in own_copies:
        for c in pair_copies:
            c.start()

    barrier = pltpu.get_barrier_semaphore()
    for k in range(1, lines):
        pl.semaphore_signal(barrier, inc=1, device_id={"seq": lax.rem(line + k, lines) * 2 + parity}, device_id_type=MESH)
    pl.semaphore_signal(barrier, inc=1, device_id={"seq": pair}, device_id_type=MESH)
    for k in range(1, n_grp):
        pl.semaphore_signal(barrier, inc=1, device_id={"grp": lax.rem(grp + k, n_grp)}, device_id_type=MESH)
    pl.semaphore_wait(barrier, lines + n_grp - 1)

    def z_copy(l, k, step):
        ref = piece(l, k, me)
        to = exchange(line, step, lines)[0] * 2 + parity
        return remote(ref, ref, z_send.at[l, k, step], z_recv.at[l, k, line], {"seq": to})

    def z_arrival(l, k, step):
        src = exchange(line, step, lines)[1]
        ref = piece(l, k, src * 2 + parity)
        return remote(ref, ref, z_send.at[l, k, step], z_recv.at[l, k, src], {"seq": src * 2 + parity})

    def y_copy(l, k, step):
        src = exchange(line, step, lines)[1]
        ref = piece(l, k, src * 2 + parity)
        return remote(ref, ref, y_send.at[l, k, src], y_recv.at[l, k, src], {"seq": pair})

    def y_arrival(l, k, step):
        src = exchange(line, step, lines)[1]
        ref = piece(l, k, src * 2 + 1 - parity)
        return remote(ref, ref, y_send.at[l, k, src], y_recv.at[l, k, src], {"seq": pair})

    order = list(range(1, lines))
    arrivals = [(k, step) for k in range(halves) for step in order]

    def send_weights(l):
        for c in own_copies[l]:
            c.wait()
        for k in range(halves + 1):
            for step in order:
                z_copy(l, k, step).start()

    def pair_weights(l):
        for k in range(halves + 1):
            y_copy(l, k, 0).start()

    def forward(l, k, step):
        z_arrival(l, k, step).wait_recv()
        y_copy(l, k, step).start()

    def ag_copy(l, k):
        to = lax.rem(grp + k, n_grp)
        return remote(xg.at[grp], xg.at[grp], ag_send.at[l, k], ag_recv.at[l, grp], {"grp": to})

    def ag_arrival(l, k):
        src = lax.rem(grp + k, n_grp)
        return remote(xg.at[src], xg.at[src], ag_send.at[l, k], ag_recv.at[l, src], {"grp": src})

    def rs_copy(l, k):
        to = lax.rem(grp + k, n_grp)
        return remote(part.at[to], rs.at[grp], rs_send.at[l, k], rs_recv.at[l, grp], {"grp": to})

    def rs_arrival(l, k):
        src = lax.rem(grp + k, n_grp)
        return remote(part.at[src], rs.at[src], rs_send.at[l, k], rs_recv.at[l, src], {"grp": src})

    def pair_copy(l):
        return remote(st_send.at[l], st_pair.at[l], p_send.at[l], p_recv.at[l], {"seq": pair})

    def line_copy(l, step):
        return remote(
            ps_send.at[l], st_line.at[l, line], l_send.at[l, step], l_recv.at[l, line],
            {"seq": lax.rem(line + step, lines) * 2 + parity},
        )

    def line_arrival(l, step):
        src = lax.rem(line + lines - step, lines)
        return remote(ps_send.at[l], st_line.at[l, src], l_send.at[l, step], l_recv.at[l, src], {"seq": src * 2 + parity})

    own_hidden.wait()
    for k in range(1, n_grp):
        ag_copy(0, k).start()
    send_weights(0)
    pair_weights(0)

    scale = head ** (-0.25)
    inv = 1.0 / math.sqrt(feats)

    def features(u, terms):
        mixed = jnp.dot(u, terms, preferred_element_type=f32)
        mixed = (mixed[:, 2 * feats :] + mixed[:, feats : 2 * feats]) + mixed[:, :feats]
        w0 = u.astype(f32) * scale
        energy = 0.5 * jnp.sum(w0 * w0, axis=-1, keepdims=True)
        return (jnp.exp(mixed - energy - stabilizer) * inv).astype(bf16)

    forwarded = 0
    for l in range(layers):
        last = l == layers - 1
        for k in range(1, n_grp):
            ag_copy(l, k).wait_send()
            ag_arrival(l, k).wait_recv()

        @pl.loop(0, tokens // 64)
        def _(t):
            at = pl.ds(pl.multiple_of(t * 64, 64), 64)
            wide = [xg[g, at, :].astype(f32) for g in range(n_grp)]
            total = sum(jnp.sum(v * v, axis=-1, keepdims=True) for v in wide)
            rms = lax.rsqrt(total / (width * n_grp) + 1e-05)
            for g in range(n_grp):
                cut = slice(g * width, (g + 1) * width)
                normed[at, cut] = (wide[g] * rms * norm_gain[l : l + 1, cut]).astype(bf16)

        for k, step in arrivals[forwarded:]:
            forward(l, k, step)
        for k in range(halves):
            for step in range(lines):
                y_arrival(l, k, step).wait_recv()

        @pl.loop(0, heads)
        def _(h):
            at = pl.ds(pl.multiple_of(h * 3 * head, 128), 3 * head)
            w = wq[l, :, :, at].reshape(n_seq * rows, 3 * head)
            qkv = jnp.dot(normed[...], w, preferred_element_type=f32).astype(bf16)
            terms = proj[l, h]
            key = features(qkv[:, head : 2 * head], terms)
            value = qkv[:, 2 * head :]
            qf[h] = features(qkv[:, :head], terms)
            kf[h] = key
            vf[h] = value
            kv = lax.dot_general(key, value, (((0,), (0,)), ((), ())), preferred_element_type=f32)
            z = jnp.dot(jnp.ones((16, tokens), bf16), key, preferred_element_type=f32)
            own_state[h, :feats] = kv
            own_state[h, feats:] = z
            st_send[l, h, :feats] = kv.astype(bf16)
            st_send[l, h, feats:] = z.astype(bf16)

        pair_copy(l).start()
        pair_copy(l).wait_recv()

        @pl.loop(0, heads)
        def _(h):
            ps_send[l, h] = (own_state[h] + st_pair[l, h].astype(f32)).astype(bf16)

        for step in range(1, lines):
            @pl.when(line + step < lines)
            def _(step=step):
                line_copy(l, step).start()

        if not last:
            send_weights(l + 1)
        for step in order:
            forward(l, halves, step)
        if not last:
            pair_weights(l + 1)

        @pl.loop(0, heads)
        def _(h):
            scores = lax.dot_general(qf[h], kf[h], (((1,), (1,)), ((), ())), preferred_element_type=f32)
            r = lax.broadcasted_iota(jnp.int32, (tokens, tokens), 0)
            c = lax.broadcasted_iota(jnp.int32, (tokens, tokens), 1)
            masked = jnp.where(r >= c, scores, 0.0)
            den[h] = jnp.broadcast_to(jnp.sum(masked, axis=-1, keepdims=True), (tokens, head))
            num[h] = jnp.dot(masked.astype(bf16), vf[h], preferred_element_type=f32)

        odd = jnp.where(parity == 1, 1.0, 0.0)

        @pl.loop(0, heads)
        def _(h):
            prefix[h] = st_pair[l, h].astype(f32) * odd

        for step in range(1, lines):
            @pl.when(line >= step)
            def _(step=step):
                line_arrival(l, step).wait_recv()
                src = lax.rem(line + lines - step, lines)

                @pl.loop(0, heads)
                def _(h):
                    prefix[h] = prefix[h] + st_line[l, src, h].astype(f32)

        @pl.loop(0, heads)
        def _(h):
            q = qf[h]
            z = prefix[h, feats : feats + 1]
            d = den[h] + jnp.sum(q.astype(f32) * z, axis=-1, keepdims=True)
            n = num[h] + jnp.dot(q, prefix[h, :feats].astype(bf16), preferred_element_type=f32)
            a = n / d
            norm = lax.rsqrt(jnp.mean(a * a, axis=-1, keepdims=True) + 1e-06)
            att[:, pl.ds(pl.multiple_of(h * head, 128), head)] = (a * norm * out_gain[l, h]).astype(bf16)

        for step in range(lines):
            y_arrival(l, halves, step).wait_recv()
        per = width // oc
        for k in list(range(1, n_grp)) + [0]:
            to = lax.rem(grp + k, n_grp)
            for i in range(per):
                part[to, :, i * oc : (i + 1) * oc] = jnp.dot(
                    att[...], wo[l, to * per + i], preferred_element_type=f32
                ).astype(bf16)
            if k:
                rs_copy(l, k).start()
        forwarded = 0
        if not last and lines > 1:
            forwarded = min(2, len(arrivals))
            for k, step in arrivals[:forwarded]:
                forward(l + 1, k, step)
        for k in range(1, n_grp):
            rs_copy(l, k).wait_send()
            rs_arrival(l, k).wait_recv()

        @pl.loop(0, tokens // 64)
        def _(t):
            at = pl.ds(pl.multiple_of(t * 64, 64), 64)
            total = part[grp, at, :].astype(f32)
            for k in range(1, n_grp):
                total = total + rs[lax.rem(grp + k, n_grp), at, :].astype(f32)
            total = (xg[grp, at, :].astype(f32) + total).astype(bf16)
            if last:
                out[at, :] = total
            else:
                xg[grp, at, :] = total

        if not last:
            for k in range(1, n_grp):
                ag_copy(l + 1, k).start()
            ready = min(4, len(arrivals))
            for k, step in arrivals[forwarded:ready]:
                forward(l + 1, k, step)
            forwarded = ready

    for l in range(layers):
        pair_copy(l).wait_send()
        for k in range(halves + 1):
            for step in range(1, lines):
                z_copy(l, k, step).wait_send()
            for step in range(lines):
                y_copy(l, k, step).wait_send()
        for step in range(1, lines):
            @pl.when(line + step < lines)
            def _(step=step):
                line_copy(l, step).wait_send()


def local(n_seq, n_grp, hidden, qkv_weight, out_weight, projection, norm_gain, out_gain):
    layers, rows, cols = qkv_weight.shape
    depth, oc = out_weight.shape[1:]
    heads, head, feats = projection.shape[1:]
    tokens, width = hidden.shape
    lines = n_seq // 2
    scaled = projection * head ** (-0.25)
    high = lax.reduce_precision(scaled, 8, 7)
    rest = scaled - high
    mid = lax.reduce_precision(rest, 8, 7)
    low = rest - mid
    terms = jnp.concatenate([high, mid, low], axis=-1).astype(bf16)
    gains = out_gain.reshape(layers, heads, 1, head)
    dma = pltpu.SemaphoreType.DMA
    vmem = pl.BlockSpec(memory_space=pltpu.VMEM)
    anywhere = pl.BlockSpec(memory_space=pl.ANY)
    state = (heads, feats + 16, head)
    return pl.pallas_call(
        functools.partial(kernel, n_seq, n_grp),
        out_shape=jax.ShapeDtypeStruct((tokens, width), bf16),
        in_specs=[anywhere, anywhere, anywhere, vmem, vmem, vmem],
        out_specs=vmem,
        scratch_shapes=[
            pltpu.VMEM((layers, n_seq, rows, cols), bf16),
            pltpu.VMEM((layers, n_seq, depth, oc), bf16),
            pltpu.VMEM((n_grp, tokens, width), bf16),
            pltpu.VMEM((n_grp, tokens, width), bf16),
            pltpu.VMEM((n_grp, tokens, width), bf16),
            pltpu.VMEM((tokens, n_grp * width), bf16),
            pltpu.VMEM((heads, tokens, feats), bf16),
            pltpu.VMEM((heads, tokens, feats), bf16),
            pltpu.VMEM((heads, tokens, head), bf16),
            pltpu.VMEM((heads, tokens, head), f32),
            pltpu.VMEM((heads, tokens, head), f32),
            pltpu.VMEM((tokens, heads * head), bf16),
            pltpu.VMEM(state, f32),
            pltpu.VMEM((layers,) + state, bf16),
            pltpu.VMEM((layers,) + state, bf16),
            pltpu.VMEM((layers,) + state, bf16),
            pltpu.VMEM((layers, lines) + state, bf16),
            pltpu.VMEM(state, f32),
            dma((1 + 2 * layers,)),
            dma((layers, 3, lines)),
            dma((layers, 3, lines)),
            dma((layers, 3, lines)),
            dma((layers, 3, lines)),
            dma((layers,)),
            dma((layers,)),
            dma((layers, lines)),
            dma((layers, lines)),
            dma((layers, n_grp)),
            dma((layers, n_grp)),
            dma((layers, n_grp)),
            dma((layers, n_grp)),
        ],
        compiler_params=pltpu.CompilerParams(
            collective_id=0, has_side_effects=True, vmem_limit_bytes=66_000_000
        ),
    )(hidden, qkv_weight, out_weight, terms, norm_gain, gains)


def solution(mesh):
    return jax.shard_map(
        functools.partial(local, mesh.shape["seq"], mesh.shape["grp"]),
        mesh=mesh,
        in_specs=(
            P("seq", "grp"),
            P(None, "seq", "grp"),
            P(None, "grp", "seq"),
            P(None, "grp", None, None),
            P(),
            P(None, "grp"),
        ),
        out_specs=P("seq", "grp"),
        check_vma=False,
    )
```
